32 devices in a mesh: slab: 32 (over z, y, x, core).
Axes of the slice: x: 2, y: 2, z: 4, core: 2. Of those that a mesh axis runs over, the one named last changes fastest.
Arguments:
- start_vectors: float32 [2, 32, 256, 256], P(None, 'slab'), may hold values from -6 to 6
- levels: int32 [32, 256, 256], P('slab'), may hold values from 0 to 15
- energies: float32 [16], replicated, may hold values from -4 to 4
Outputs:
- cheb_field: float32 [2, 32, 256, 256], P(None, 'slab')
- lanczos_diag: float32 [2, 8], replicated
- lanczos_off: float32 [2, 7], replicated
- moments: float32 [2, 6], replicated
The draws below stay inside these ranges and needn't reach their ends.
All inputs are finite; a program needn't handle non-finite values.
Results may differ from the reference program's by a relative error of at most 0.0001.
Values sent between devices are 32-bit elements; how exact they have to be, the bound alone decides.
A program may use at most 64 MiB of HBM per device.

```python
import jax
import jax.numpy as jnp
from jax import lax

NY = 256
NX = 256
VECS = 2
LANCZOS = 8
LEVELS = 16
NZ = 32


def place_ends(entries, stream_key, low, largest):
    shape = entries.shape
    index_at = [jax.random.randint(jax.random.fold_in(stream_key, axis), (), 0, shape[axis]) for axis in range(len(shape))]
    entries = entries.at[tuple(index_at)].set(low)
    longest = shape.index(max(shape))
    index_at[longest] = (index_at[longest] + 1) % shape[longest]
    return entries.at[tuple(index_at)].set(largest)


def shard_levels(stream_key, shape, cuts, least, largest):
    loudness = 1.0
    for position, blocks in cuts:
        heights = jax.random.uniform(jax.random.fold_in(jax.random.fold_in(stream_key, 6), position), (blocks,), jnp.float32, least / len(cuts), largest / len(cuts))
        loudness = loudness * jnp.repeat(jnp.exp(heights), shape[position] // blocks).reshape((-1,) + (1,) * (len(shape) - 1 - position))
    return loudness


def normal_values(stream_key, extent, spread, most, shards=(), held_as=jnp.bfloat16):
    array = spread * jax.random.normal(stream_key, extent, jnp.float32)
    if shards:
        array = array * shard_levels(stream_key, extent, shards, -0.22, 0.18)
    return jnp.clip(array, -most, most).astype(held_as)


def setup_inputs(seed: int = 0) -> dict:
    arg_keys = jax.random.split(jax.random.key(seed), 4)
    return {
        "start_vectors": normal_values(arg_keys[0], (VECS, NZ, NY, NX), 1.0, 6.0, ((1, 32),), jnp.float32),
        "levels": place_ends(jax.random.randint(arg_keys[1], (NZ, NY, NX), 0, LEVELS), jax.random.fold_in(arg_keys[1], 1), 0, LEVELS - 1).astype(jnp.int32),
        "energies": jnp.clip(jax.random.uniform(arg_keys[2], (LEVELS,), jnp.float32, -4.0, 4.0), -4.0, 4.0),
    }


def hamiltonian(field, onsite):
    beside = jnp.roll(field, 1, 1) + jnp.roll(field, -1, 1)
    beside = beside + jnp.roll(field, 1, 2) + jnp.roll(field, -1, 2)
    beside = beside + jnp.roll(field, 1, 3) + jnp.roll(field, -1, 3)
    return onsite[None] * field - beside

def inner(first, second):
    return lax.optimization_barrier(jnp.sum(first * second, axis=(1, 2, 3)))

def expand(values):
    return values[:, None, None, None]

def reference(start_vectors, levels, energies):
    onsite = jnp.take(energies, levels, axis=0)
    norm0 = inner(start_vectors, start_vectors)
    vector = start_vectors / expand(jnp.sqrt(norm0))
    previous = jnp.zeros_like(vector)
    beta_prev = jnp.zeros((VECS,), jnp.float32)
    alphas = []
    betas = []
    for step in range(LANCZOS):
        work = hamiltonian(vector, onsite) - expand(beta_prev) * previous
        alpha = inner(vector, work)
        alphas.append(alpha)
        if step < LANCZOS - 1:
            work = work - expand(alpha) * vector
            beta = jnp.sqrt(inner(work, work))
            betas.append(beta)
            previous, vector, beta_prev = (vector, work / expand(beta), beta)
    diag = jnp.stack(alphas, axis=1)
    offd = jnp.stack(betas, axis=1)
    zero_col = jnp.zeros((VECS, 1), jnp.float32)
    left = jnp.concatenate([zero_col, offd], axis=1)
    right = jnp.concatenate([offd, zero_col], axis=1)
    emin = lax.optimization_barrier(jnp.min(diag - left - right, axis=1))
    emax = lax.optimization_barrier(jnp.max(diag + left + right, axis=1))
    center = expand((emax + emin) * 0.5)
    half = expand(0.55 * (emax - emin))

    def scaled(field):
        return (hamiltonian(field, onsite) - center * field) / half
    term0 = start_vectors
    term1 = scaled(term0)
    term2 = 2.0 * scaled(term1) - term0
    term3 = 2.0 * scaled(term2) - term1
    first = inner(term0, term1)
    moments = jnp.stack([first, inner(term0, term2), inner(term0, term3), 2.0 * inner(term2, term2) - norm0, 2.0 * inner(term3, term2) - first, 2.0 * inner(term3, term3) - norm0], axis=1) / norm0[:, None]
    return (term3, diag, offd, moments)
```

```python
import functools

import jax
import jax.numpy as jnp
from jax import lax
from jax.experimental import pallas as pl
from jax.experimental.pallas import tpu as pltpu
from jax.sharding import PartitionSpec as P

LANCZOS = 8
HALF = LANCZOS // 2
GROUP = 8
GHOST = 8
RETURNED = 3


def phase_one(dots, half, sqrt):
    norm = dots[0]
    nu = [None] * len(dots)
    nu[0] = norm / norm
    nu[1] = dots[1] / norm
    for k in range(2, len(dots)):
        nu[k] = 2.0 * dots[k] / norm - nu[k % 2]
    top = len(nu) - 1
    row, before = list(nu), None
    diag, offd = [], []
    for k in range(half):
        if k == 0:
            alpha = row[1]
        else:
            alpha = (0.5 * row[k + 1] - offd[-1] * before[k]) / row[k]
        diag.append(alpha)
        new = [None] * len(nu)
        for l in range(k + 1, top - k):
            new[l] = 0.5 * (row[l + 1] + row[l - 1]) - alpha * row[l]
            if k:
                new[l] = new[l] - offd[-1] * before[l]
        beta = sqrt(new[k + 1] / (row[k] if k == 0 else 2.0 * row[k]))
        offd.append(beta)
        inv = 1.0 / beta
        before, row = row, [None if x is None else x * inv for x in new]
    zero = nu[0] * 0.0
    scale = 1.0 / sqrt(norm)
    vectors = [[scale] + [zero] * half]
    for k in range(half):
        now = vectors[-1]
        inv = 1.0 / offd[k]
        shifted = [zero] * (half + 1)
        for l in range(k + 1):
            if l == 0:
                shifted[1] = shifted[1] + now[0]
            else:
                shifted[l + 1] = shifted[l + 1] + 0.5 * now[l]
                shifted[l - 1] = shifted[l - 1] + 0.5 * now[l]
        new = [shifted[l] - diag[k] * now[l] for l in range(half + 1)]
        if k:
            new = [x - offd[k - 1] * y for x, y in zip(new, vectors[-2])]
        vectors.append([x * inv for x in new])
    return nu, diag, offd, vectors


def phase_two(dots, diag, offd, half, sqrt):
    count = len(dots)
    gram = {}
    for k, value in enumerate(dots):
        gram[(half + k // 2, half + (k + 1) // 2)] = value
    zero = dots[0] * 0.0
    one = zero + 1.0
    for k in range(half):
        gram[(k, half)] = zero
        gram[(k, half - 1)] = one if k == half - 1 else zero
    guess_a, guess_b = diag[half - 1], offd[half - 1]
    inv = 1.0 / guess_b

    def entry(i, j):
        if (i, j) in gram:
            return gram[(i, j)]
        if j > half and i < half and (j - half) < (half - i) + 1:
            value = zero
        elif i >= half:
            value = entry(i + 1, j - 1) + entry(i - 1, j - 1) - entry(i, j - 2)
        else:
            value = (offd[i] * inv) * entry(i + 1, j - 1) - entry(i, j - 2)
            if i != half - 1:
                value = value + ((diag[i] - guess_a) * inv) * entry(i, j - 1)
            if i > 0:
                value = value + (offd[i - 1] * inv) * entry(i - 1, j - 1)
        gram[(i, j)] = value
        return value

    top = half + count - 1
    row = {l: entry(half, l) for l in range(half, top + 1)}
    before = {l: entry(half - 1, l) for l in range(half, top)}
    diag, offd = list(diag), list(offd)
    for k in range(half, 2 * half):
        if k == half:
            alpha = guess_a + guess_b * row[k + 1] / row[k]
        else:
            alpha = guess_a + (guess_b * row[k + 1] - offd[k - 1] * before[k]) / row[k]
        diag.append(alpha)
        if k == 2 * half - 1:
            break
        new = {}
        for l in range(k + 1, top - (k - half)):
            new[l] = guess_b * (row[l + 1] + row[l - 1]) + (guess_a - alpha) * row[l] - offd[k - 1] * before[l]
        beta = sqrt(new[k + 1] * guess_b / row[k])
        offd.append(beta)
        inv_b = 1.0 / beta
        before, row = row, {l: x * inv_b for l, x in new.items()}
    return diag, offd


def chebyshev(diag, offd, nu, centre, width):
    left = [None] + offd
    right = offd + [None]
    low, high = None, None
    for a, b, c in zip(diag, left, right):
        reach = b if c is None else c if b is None else b + c
        low = a - reach if low is None else jnp.minimum(low, a - reach)
        high = a + reach if high is None else jnp.maximum(high, a + reach)
    inv = 1.0 / (0.55 * (high - low))
    al = width * inv
    be = (centre - 0.5 * (high + low)) * inv
    p, q, r = 2.0 * be * be + al * al - 1.0, 4.0 * al * be, al * al
    first = [be, al]
    second = [p, q, r]
    third = [2.0 * be * p + al * q - be, 2.0 * be * q + al * (2.0 * p + r) - al, 2.0 * be * r + al * q, al * r]

    def dot(f, g):
        total = None
        for i, x in enumerate(f):
            for j, y in enumerate(g):
                term = (x * y) * (0.5 * (nu[i + j] + nu[abs(i - j)]))
                total = term if total is None else total + term
        return total

    start = [nu[0]]
    m1 = dot(start, first)
    moments = [
        m1,
        dot(start, second),
        dot(start, third),
        2.0 * dot(second, second) - 1.0,
        2.0 * dot(third, second) - m1,
        2.0 * dot(third, third) - 1.0,
    ]
    return third, moments


def kernel(
    count, energies, start, levels, cheb, diag_out, offd_out, moments_out,
    own, own_levels, field, halo, onsite, level, back, part, part_far, mine,
    load_sem, vec_sem, level_sem, halo_send, halo_recv, back_send, back_recv, red_send, red_recv,
):
    me = lax.axis_index("slab")
    member = lax.rem(me, GROUP)
    group = me // GROUP
    base = me - member
    groups = count // GROUP
    vecs, _, height, lanes = start.shape
    rows = height // GROUP
    deep = rows + 2 * GHOST
    mesh_id = pl.DeviceIdType.MESH
    ahead = lax.rem(me + GROUP, count)
    behind = lax.rem(me + count - GROUP, count)

    loads = [
        pltpu.make_async_copy(start.at[:, 0], own, load_sem.at[0]),
        pltpu.make_async_copy(levels.at[0], own_levels, load_sem.at[1]),
    ]
    for copy in loads:
        copy.start()

    def peer(i):
        return base + lax.rem(member + i, GROUP)

    def far(i):
        return lax.rem(me + i * GROUP, count)

    barrier = pltpu.get_barrier_semaphore()

    def greet(i, carry):
        pl.semaphore_signal(barrier, inc=1, device_id=(peer(i),), device_id_type=mesh_id)
        return carry

    def greet_far(i, carry):
        pl.semaphore_signal(barrier, inc=1, device_id=(far(i),), device_id_type=mesh_id)
        return carry

    lax.fori_loop(1, GROUP, greet, 0)
    lax.fori_loop(1, groups, greet_far, 0)
    pl.semaphore_wait(barrier, GROUP - 1 + groups - 1)

    def pieces(i):
        mid = pl.multiple_of(i * rows, 8)
        top = pl.multiple_of(lax.rem(i * rows + height - GHOST, height), 8)
        low = pl.multiple_of(lax.rem(i * rows + rows, height), 8)
        return ((mid, GHOST, rows), (top, 0, GHOST), (low, GHOST + rows, GHOST))

    def vec_refs(i):
        return [
            (own.at[:, pl.ds(at, size)], field.at[0, :, member, pl.ds(to, size)])
            for at, to, size in pieces(i)
        ]

    def level_refs(i):
        return [
            (own_levels.at[pl.ds(at, size)], level.at[member, pl.ds(to, size)])
            for at, to, size in pieces(i)
        ]

    def scatter(refs, sems):
        def body(i, carry):
            to = lax.rem(member + i, GROUP)
            for src, dst in refs(to):
                pltpu.make_async_remote_copy(
                    src_ref=src, dst_ref=dst, send_sem=sems.at[0], recv_sem=sems.at[1],
                    device_id=(base + to,), device_id_type=mesh_id,
                ).start()
            return carry

        lax.fori_loop(1, GROUP, body, 0)
        for src, dst in refs(member):
            pltpu.make_async_copy(src, dst, sems.at[1]).start()

    def drain(ref, sem):
        pltpu.make_async_copy(ref, ref, sem).wait()

    loads[0].wait()
    scatter(vec_refs, vec_sem)
    loads[1].wait()
    scatter(level_refs, level_sem)

    values = [energies[i] for i in range(energies.shape[0])]
    mean = sum(values[1:], values[0]) * (1.0 / len(values))
    spread = [(x - mean) * (x - mean) for x in values]
    spread = sum(spread[1:], spread[0]) * (1.0 / len(values))
    width = 2.0 * jnp.sqrt(jnp.full((1, lanes), spread + 6.0, jnp.float32))
    inv_width = 1.0 / width

    def halo_copies(slot, at):
        return [
            pltpu.make_async_remote_copy(
                src_ref=field.at[slot, :, plane], dst_ref=halo.at[at, side],
                send_sem=halo_send.at[at, side], recv_sem=halo_recv.at[at, side],
                device_id=(to,), device_id_type=mesh_id,
            )
            for plane, side, to in ((0, 1, behind), (GROUP - 1, 0, ahead))
        ]

    def give_back(k):
        def refs(i):
            return (
                field.at[k, :, i, pl.ds(GHOST, rows)],
                back.at[k - 1, :, pl.ds(pl.multiple_of(member * rows, 8), rows)],
            )

        def body(i, carry):
            to = lax.rem(member + i, GROUP)
            src, dst = refs(to)
            pltpu.make_async_remote_copy(
                src_ref=src, dst_ref=dst, send_sem=back_send.at[k - 1], recv_sem=back_recv.at[k - 1],
                device_id=(base + to,), device_id_type=mesh_id,
            ).start()
            return carry

        lax.fori_loop(1, GROUP, body, 0)
        src, dst = refs(member)
        pltpu.make_async_copy(src, dst, back_recv.at[k - 1]).start()

    def tile_sum(x):
        x = x[GHOST : GHOST + rows]
        total = x[0:8]
        for i in range(8, rows, 8):
            total = total + x[i : i + 8]
        return total

    def step(source, target, before, at, combine, extra=False):
        nothing = jnp.zeros((8, lanes), jnp.float32)

        def plane(m, below, above, sums):
            sums = list(sums)
            for v in range(vecs):
                here = field[source, v, m]
                near = pltpu.roll(here, 1, 0) + pltpu.roll(here, deep - 1, 0)
                near = near + pltpu.roll(here, 1, 1) + pltpu.roll(here, lanes - 1, 1)
                near = near + below(v) + above(v)
                applied = onsite[m] * here - inv_width * near
                new = combine(v, applied, here, None if before is None else field[before, v, m])
                if target is not None:
                    field[target, v, m] = new
                sums[3 * v] = sums[3 * v] + tile_sum(here * new)
                sums[3 * v + 1] = sums[3 * v + 1] + tile_sum(new * new)
                if extra:
                    sums[3 * v + 2] = sums[3 * v + 2] + tile_sum(here * here)
            return tuple(sums)

        sums = (nothing,) * (3 * vecs)
        sums = plane(0, lambda v: halo[at, 0, v], lambda v: field[source, v, 1], sums)
        sums = plane(
            GROUP - 1, lambda v: field[source, v, GROUP - 2], lambda v: halo[at, 1, v], sums
        )
        sent = []
        if target is not None:
            sent = halo_copies(target, at + 1)
            for copy in sent:
                copy.start()
        sums = lax.fori_loop(
            1,
            GROUP - 1,
            lambda m, carry: plane(
                m, lambda v: field[source, v, m - 1], lambda v: field[source, v, m + 1], carry
            ),
            sums,
        )
        return sums, sent

    lane = lax.broadcasted_iota(jnp.int32, (8, 128), 1)
    line = lax.broadcasted_iota(jnp.int32, (8, 128), 0)

    def reduce_all(dots, turn):
        tile = jnp.zeros((8, 128), jnp.float32)
        for d, per_vec in enumerate(dots):
            for v, value in enumerate(per_vec):
                whole = jnp.sum(jnp.sum(value, axis=0, keepdims=True), axis=1, keepdims=True)
                tile = jnp.where((lane == d) & (line == v), whole, tile)
        for leg, (slots, index, size, target) in enumerate(
            ((part.at[turn], member, GROUP, peer), (part_far.at[turn], group, groups, far))
        ):
            mine[turn, leg] = tile
            slots[index] = tile

            def body(i, carry):
                pltpu.make_async_remote_copy(
                    src_ref=mine.at[turn, leg], dst_ref=slots.at[index],
                    send_sem=red_send.at[turn, leg], recv_sem=red_recv.at[turn, leg],
                    device_id=(target(i),), device_id_type=mesh_id,
                ).start()
                return carry

            lax.fori_loop(1, size, body, 0)
            drain(slots.at[pl.ds(0, size - 1)], red_recv.at[turn, leg])
            tile = slots[0]
            for i in range(1, size):
                tile = tile + slots[i]
        return [
            jnp.broadcast_to(tile[0:vecs, d : d + 1], (vecs, lanes)) for d in range(len(dots))
        ]

    drain(field.at[0], vec_sem.at[1])
    sent = [halo_copies(0, 0)]
    for copy in sent[0]:
        copy.start()
    drain(level, level_sem.at[1])

    def look_up(m, carry):
        ids = level[m]
        energy = jnp.full(ids.shape, values[0] - mean, jnp.float32)
        for i in range(1, len(values)):
            energy = jnp.where(ids == i, values[i] - mean, energy)
        onsite[m] = energy * inv_width
        return carry

    lax.fori_loop(0, GROUP, look_up, 0)

    def arrive(copies):
        for copy in copies:
            copy.wait_recv()

    dots = [None]
    for k in range(HALF):
        arrive(sent[k])
        if k == 0:
            rule = lambda v, applied, here, old: applied
        else:
            rule = lambda v, applied, here, old: 2.0 * applied - old
        sums, copies = step(k, k + 1, k - 1 if k else None, k, rule, extra=k == 0)
        sent.append(copies)
        if k == 0:
            dots[0] = [sums[3 * v + 2] for v in range(vecs)]
        dots.append([sums[3 * v] for v in range(vecs)])
        dots.append([sums[3 * v + 1] for v in range(vecs)])
        if k + 1 <= RETURNED:
            give_back(k + 1)

    totals = reduce_all(dots, 0)
    nu, diag, offd, vectors = phase_one(totals, HALF, jnp.sqrt)
    arrive(sent[HALF])
    old_at, new_at = HALF + 1, HALF + 2

    def mix(coefficients, v, read):
        total = coefficients[0][v : v + 1] * read(0)
        for k in range(1, len(coefficients)):
            total = total + coefficients[k][v : v + 1] * read(k)
        return total

    old_mix, new_mix = vectors[HALF - 1][:HALF], vectors[HALF]
    for side in range(2):
        for v in range(vecs):
            halo[HALF, side, v] = mix(new_mix, v, lambda k: halo[k, side, v])

    def restart(m, sums):
        sums = list(sums)
        for v in range(vecs):
            field[old_at, v, m] = mix(old_mix, v, lambda k: field[k, v, m])
            new = mix(new_mix, v, lambda k: field[k, v, m])
            field[new_at, v, m] = new
            sums[v] = sums[v] + tile_sum(new * new)
        return tuple(sums)

    sums = lax.fori_loop(0, GROUP, restart, (jnp.zeros((8, lanes), jnp.float32),) * vecs)
    dots = [list(sums)]
    gain = 1.0 / offd[HALF - 1]
    shift = diag[HALF - 1]

    def rule(v, applied, here, old):
        return gain[v : v + 1] * (applied - shift[v : v + 1] * here) - old

    for k in range(HALF):
        at = HALF + k
        if k:
            arrive(sent[at])
        last = k == HALF - 1
        sums, copies = step(new_at + k, None if last else new_at + k + 1, new_at + k - 1, at, rule)
        sent.append(copies)
        dots.append([sums[3 * v] for v in range(vecs)])
        if not last:
            dots.append([sums[3 * v + 1] for v in range(vecs)])

    totals = reduce_all(dots, 1)
    diag, offd = phase_two(totals, diag, offd, HALF, jnp.sqrt)
    diag = [width * a + mean for a in diag]
    offd = [width * b for b in offd]
    third, moments = chebyshev(diag, offd, nu, mean, width)

    for k in range(RETURNED):
        drain(back.at[k], back_recv.at[k])
    for v in range(vecs):
        cheb[v, 0] = mix(third, v, lambda k: own[v] if k == 0 else back[k - 1, v])

    for ref, items in ((diag_out, diag), (offd_out, offd), (moments_out, moments)):
        at = lax.broadcasted_iota(jnp.int32, ref.shape, 1)
        value = jnp.zeros(ref.shape, jnp.float32)
        for i, item in enumerate(items):
            value = jnp.where(at == i, item[:, : ref.shape[1]], value)
        ref[...] = value

    for copies in sent:
        for copy in copies:
            copy.wait_send()
    drain(field.at[0, :, pl.ds(0, GROUP - 1)], vec_sem.at[0])
    drain(level.at[pl.ds(0, GROUP - 1)], level_sem.at[0])
    for k in range(RETURNED):
        drain(field.at[k + 1, :, pl.ds(0, GROUP - 1), pl.ds(GHOST, rows)], back_send.at[k])
    for turn in range(2):
        drain(part.at[turn, pl.ds(0, GROUP - 1)], red_send.at[turn, 0])
        drain(part_far.at[turn, pl.ds(0, groups - 1)], red_send.at[turn, 1])


def shards(count, start_vectors, levels, energies):
    vecs, _, height, lanes = start_vectors.shape
    groups = count // GROUP
    deep = height // GROUP + 2 * GHOST
    f32 = jnp.float32
    vmem = pl.BlockSpec(memory_space=pltpu.VMEM)
    anywhere = pl.BlockSpec(memory_space=pl.ANY)
    dma = pltpu.SemaphoreType.DMA
    return pl.pallas_call(
        functools.partial(kernel, count),
        out_shape=(
            jax.ShapeDtypeStruct(start_vectors.shape, f32),
            jax.ShapeDtypeStruct((vecs, LANCZOS), f32),
            jax.ShapeDtypeStruct((vecs, LANCZOS - 1), f32),
            jax.ShapeDtypeStruct((vecs, 6), f32),
        ),
        in_specs=[pl.BlockSpec(memory_space=pltpu.SMEM), anywhere, anywhere],
        out_specs=(vmem,) * 4,
        scratch_shapes=[
            pltpu.VMEM((vecs, height, lanes), f32),
            pltpu.VMEM((height, lanes), jnp.int32),
            pltpu.VMEM((LANCZOS + 2, vecs, GROUP, deep, lanes), f32),
            pltpu.VMEM((LANCZOS, 2, vecs, deep, lanes), f32),
            pltpu.VMEM((GROUP, deep, lanes), f32),
            pltpu.VMEM((GROUP, deep, lanes), jnp.int32),
            pltpu.VMEM((RETURNED, vecs, height, lanes), f32),
            pltpu.VMEM((2, GROUP, 8, 128), f32),
            pltpu.VMEM((2, groups, 8, 128), f32),
            pltpu.VMEM((2, 2, 8, 128), f32),
            dma((2,)),
            dma((2,)),
            dma((2,)),
            dma((LANCZOS, 2)),
            dma((LANCZOS, 2)),
            dma((RETURNED,)),
            dma((RETURNED,)),
            dma((2, 2)),
            dma((2, 2)),
        ],
        compiler_params=pltpu.CompilerParams(
            collective_id=0, has_side_effects=True, vmem_limit_bytes=48 * 1024 * 1024
        ),
    )(energies, start_vectors, levels)


def solution(mesh):
    in_specs = (P(None, "slab", None, None), P("slab", None, None), P())
    out_specs = (P(None, "slab", None, None), P(), P(), P())
    return jax.shard_map(
        functools.partial(shards, mesh.shape["slab"]),
        mesh=mesh, in_specs=in_specs, out_specs=out_specs, check_vma=False,
    )
```

```python
import functools

import jax
import jax.numpy as jnp
from jax import lax
from jax.experimental import pallas as pl
from jax.experimental.pallas import tpu as pltpu
from jax.sharding import PartitionSpec as P

LANCZOS = 8
HALF = LANCZOS // 2
GROUP = 8
GHOST = 8
RETURNED = 3


def phase_one(dots, half, sqrt):
    norm = dots[0]
    nu = [None] * len(dots)
    nu[0] = norm / norm
    nu[1] = dots[1] / norm
    for k in range(2, len(dots)):
        nu[k] = 2.0 * dots[k] / norm - nu[k % 2]
    top = len(nu) - 1
    row, before = list(nu), None
    diag, offd = [], []
    for k in range(half):
        if k == 0:
            alpha = row[1]
        else:
            alpha = (0.5 * row[k + 1] - offd[-1] * before[k]) / row[k]
        diag.append(alpha)
        new = [None] * len(nu)
        for l in range(k + 1, top - k):
            new[l] = 0.5 * (row[l + 1] + row[l - 1]) - alpha * row[l]
            if k:
                new[l] = new[l] - offd[-1] * before[l]
        beta = sqrt(new[k + 1] / (row[k] if k == 0 else 2.0 * row[k]))
        offd.append(beta)
        inv = 1.0 / beta
        before, row = row, [None if x is None else x * inv for x in new]
    zero = nu[0] * 0.0
    scale = 1.0 / sqrt(norm)
    vectors = [[scale] + [zero] * half]
    for k in range(half):
        now = vectors[-1]
        inv = 1.0 / offd[k]
        shifted = [zero] * (half + 1)
        for l in range(k + 1):
            if l == 0:
                shifted[1] = shifted[1] + now[0]
            else:
                shifted[l + 1] = shifted[l + 1] + 0.5 * now[l]
                shifted[l - 1] = shifted[l - 1] + 0.5 * now[l]
        new = [shifted[l] - diag[k] * now[l] for l in range(half + 1)]
        if k:
            new = [x - offd[k - 1] * y for x, y in zip(new, vectors[-2])]
        vectors.append([x * inv for x in new])
    return nu, diag, offd, vectors


def phase_two(dots, diag, offd, half, sqrt):
    count = len(dots)
    gram = {}
    for k, value in enumerate(dots):
        gram[(half + k // 2, half + (k + 1) // 2)] = value
    zero = dots[0] * 0.0
    one = zero + 1.0
    for k in range(half):
        gram[(k, half)] = zero
        gram[(k, half - 1)] = one if k == half - 1 else zero
    guess_a, guess_b = diag[half - 1], offd[half - 1]
    inv = 1.0 / guess_b

    def entry(i, j):
        if (i, j) in gram:
            return gram[(i, j)]
        if j > half and i < half and (j - half) < (half - i) + 1:
            value = zero
        elif i >= half:
            value = entry(i + 1, j - 1) + entry(i - 1, j - 1) - entry(i, j - 2)
        else:
            value = (offd[i] * inv) * entry(i + 1, j - 1) - entry(i, j - 2)
            if i != half - 1:
                value = value + ((diag[i] - guess_a) * inv) * entry(i, j - 1)
            if i > 0:
                value = value + (offd[i - 1] * inv) * entry(i - 1, j - 1)
        gram[(i, j)] = value
        return value

    top = half + count - 1
    row = {l: entry(half, l) for l in range(half, top + 1)}
    before = {l: entry(half - 1, l) for l in range(half, top)}
    diag, offd = list(diag), list(offd)
    for k in range(half, 2 * half):
        if k == half:
            alpha = guess_a + guess_b * row[k + 1] / row[k]
        else:
            alpha = guess_a + (guess_b * row[k + 1] - offd[k - 1] * before[k]) / row[k]
        diag.append(alpha)
        if k == 2 * half - 1:
            break
        new = {}
        for l in range(k + 1, top - (k - half)):
            new[l] = guess_b * (row[l + 1] + row[l - 1]) + (guess_a - alpha) * row[l] - offd[k - 1] * before[l]
        beta = sqrt(new[k + 1] * guess_b / row[k])
        offd.append(beta)
        inv_b = 1.0 / beta
        before, row = row, {l: x * inv_b for l, x in new.items()}
    return diag, offd


def chebyshev(diag, offd, nu, centre, width):
    left = [None] + offd
    right = offd + [None]
    low, high = None, None
    for a, b, c in zip(diag, left, right):
        reach = b if c is None else c if b is None else b + c
        low = a - reach if low is None else jnp.minimum(low, a - reach)
        high = a + reach if high is None else jnp.maximum(high, a + reach)
    inv = 1.0 / (0.55 * (high - low))
    al = width * inv
    be = (centre - 0.5 * (high + low)) * inv
    p, q, r = 2.0 * be * be + al * al - 1.0, 4.0 * al * be, al * al
    first = [be, al]
    second = [p, q, r]
    third = [2.0 * be * p + al * q - be, 2.0 * be * q + al * (2.0 * p + r) - al, 2.0 * be * r + al * q, al * r]

    def dot(f, g):
        total = None
        for i, x in enumerate(f):
            for j, y in enumerate(g):
                term = (x * y) * (0.5 * (nu[i + j] + nu[abs(i - j)]))
                total = term if total is None else total + term
        return total

    start = [nu[0]]
    m1 = dot(start, first)
    moments = [
        m1,
        dot(start, second),
        dot(start, third),
        2.0 * dot(second, second) - 1.0,
        2.0 * dot(third, second) - m1,
        2.0 * dot(third, third) - 1.0,
    ]
    return third, moments


def kernel(
    count, energies, start, levels, cheb, diag_out, offd_out, moments_out,
    own, own_levels, field, halo, onsite, level, back, part, part_far, mine,
    load_sem, vec_sem, level_sem, halo_send, halo_recv, back_send, back_recv, red_send, red_recv,
):
    me = lax.axis_index("slab")
    member = lax.rem(me, GROUP)
    group = me // GROUP
    base = me - member
    groups = count // GROUP
    vecs, _, height, lanes = start.shape
    my_vec, block = lax.rem(member, vecs), member // vecs
    rows = height // (GROUP // vecs)
    deep = rows + 2 * GHOST
    mesh_id = pl.DeviceIdType.MESH
    ahead = lax.rem(me + GROUP, count)
    behind = lax.rem(me + count - GROUP, count)

    loads = [
        pltpu.make_async_copy(start.at[:, 0], own, load_sem.at[0]),
        pltpu.make_async_copy(levels.at[0], own_levels, load_sem.at[1]),
    ]
    for copy in loads:
        copy.start()

    def peer(i):
        return base + lax.rem(member + i, GROUP)

    def far(i):
        return lax.rem(me + i * GROUP, count)

    barrier = pltpu.get_barrier_semaphore()

    def greet(i, carry):
        pl.semaphore_signal(barrier, inc=1, device_id=(peer(i),), device_id_type=mesh_id)
        return carry

    def greet_far(i, carry):
        pl.semaphore_signal(barrier, inc=1, device_id=(far(i),), device_id_type=mesh_id)
        return carry

    lax.fori_loop(1, GROUP, greet, 0)
    lax.fori_loop(1, groups, greet_far, 0)
    pl.semaphore_wait(barrier, GROUP - 1 + groups - 1)

    def pieces(i):
        i = i // vecs
        mid = pl.multiple_of(i * rows, 8)
        top = pl.multiple_of(lax.rem(i * rows + height - GHOST, height), 8)
        low = pl.multiple_of(lax.rem(i * rows + rows, height), 8)
        return ((mid, GHOST, rows), (top, 0, GHOST), (low, GHOST + rows, GHOST))

    def vec_refs(i):
        return [
            (own.at[lax.rem(i, vecs), pl.ds(at, size)], field.at[0, member, pl.ds(to, size)])
            for at, to, size in pieces(i)
        ]

    def level_refs(i):
        return [
            (own_levels.at[pl.ds(at, size)], level.at[member, pl.ds(to, size)])
            for at, to, size in pieces(i)
        ]

    def scatter(refs, sems):
        def body(i, carry):
            to = lax.rem(member + i, GROUP)
            for src, dst in refs(to):
                pltpu.make_async_remote_copy(
                    src_ref=src, dst_ref=dst, send_sem=sems.at[0], recv_sem=sems.at[1],
                    device_id=(base + to,), device_id_type=mesh_id,
                ).start()
            return carry

        lax.fori_loop(1, GROUP, body, 0)
        for src, dst in refs(member):
            pltpu.make_async_copy(src, dst, sems.at[1]).start()

    def drain(ref, sem):
        pltpu.make_async_copy(ref, ref, sem).wait()

    loads[0].wait()
    scatter(vec_refs, vec_sem)
    loads[1].wait()
    scatter(level_refs, level_sem)

    values = [energies[i] for i in range(energies.shape[0])]
    mean = sum(values[1:], values[0]) * (1.0 / len(values))
    spread = [(x - mean) * (x - mean) for x in values]
    spread = sum(spread[1:], spread[0]) * (1.0 / len(values))
    width = 2.0 * jnp.sqrt(jnp.full((1, lanes), spread + 6.0, jnp.float32))
    inv_width = 1.0 / width

    def halo_copies(slot, at):
        return [
            pltpu.make_async_remote_copy(
                src_ref=field.at[slot, plane], dst_ref=halo.at[at, side],
                send_sem=halo_send.at[at, side], recv_sem=halo_recv.at[at, side],
                device_id=(to,), device_id_type=mesh_id,
            )
            for plane, side, to in ((0, 1, behind), (GROUP - 1, 0, ahead))
        ]

    def give_back(k):
        def refs(i):
            return (
                field.at[k, i, pl.ds(GHOST, rows)],
                back.at[k - 1, my_vec, pl.ds(pl.multiple_of(block * rows, 8), rows)],
            )

        def body(i, carry):
            to = lax.rem(member + i, GROUP)
            src, dst = refs(to)
            pltpu.make_async_remote_copy(
                src_ref=src, dst_ref=dst, send_sem=back_send.at[k - 1], recv_sem=back_recv.at[k - 1],
                device_id=(base + to,), device_id_type=mesh_id,
            ).start()
            return carry

        lax.fori_loop(1, GROUP, body, 0)
        src, dst = refs(member)
        pltpu.make_async_copy(src, dst, back_recv.at[k - 1]).start()

    def tile_sum(x):
        x = x[GHOST : GHOST + rows]
        total = x[0:8]
        for i in range(8, rows, 8):
            total = total + x[i : i + 8]
        return total

    def step(source, target, before, at, combine, extra=False):
        nothing = jnp.zeros((8, lanes), jnp.float32)

        def plane(m, below, above, sums):
            sums = list(sums)
            here = field[source, m]
            near = pltpu.roll(here, 1, 0) + pltpu.roll(here, deep - 1, 0)
            near = near + pltpu.roll(here, 1, 1) + pltpu.roll(here, lanes - 1, 1)
            near = near + below() + above()
            applied = onsite[m] * here - inv_width * near
            new = combine(applied, here, None if before is None else field[before, m])
            if target is not None:
                field[target, m] = new
            sums[0] = sums[0] + tile_sum(here * new)
            sums[1] = sums[1] + tile_sum(new * new)
            if extra:
                sums[2] = sums[2] + tile_sum(here * here)
            return tuple(sums)

        sums = (nothing,) * 3
        sums = plane(0, lambda: halo[at, 0], lambda: field[source, 1], sums)
        sums = plane(GROUP - 1, lambda: field[source, GROUP - 2], lambda: halo[at, 1], sums)
        sent = []
        if target is not None:
            sent = halo_copies(target, at + 1)
            for copy in sent:
                copy.start()
        sums = lax.fori_loop(
            1,
            GROUP - 1,
            lambda m, carry: plane(
                m, lambda: field[source, m - 1], lambda: field[source, m + 1], carry
            ),
            sums,
        )
        return sums, sent

    lane = lax.broadcasted_iota(jnp.int32, (8, 128), 1)
    line = lax.broadcasted_iota(jnp.int32, (8, 128), 0)

    def reduce_all(dots, turn):
        tile = jnp.zeros((8, 128), jnp.float32)
        for d, value in enumerate(dots):
            whole = jnp.sum(jnp.sum(value, axis=0, keepdims=True), axis=1, keepdims=True)
            tile = jnp.where((lane == d) & (line == my_vec), whole, tile)
        for leg, (slots, index, size, target) in enumerate(
            ((part.at[turn], member, GROUP, peer), (part_far.at[turn], group, groups, far))
        ):
            mine[turn, leg] = tile
            slots[index] = tile

            def body(i, carry):
                pltpu.make_async_remote_copy(
                    src_ref=mine.at[turn, leg], dst_ref=slots.at[index],
                    send_sem=red_send.at[turn, leg], recv_sem=red_recv.at[turn, leg],
                    device_id=(target(i),), device_id_type=mesh_id,
                ).start()
                return carry

            lax.fori_loop(1, size, body, 0)
            drain(slots.at[pl.ds(0, size - 1)], red_recv.at[turn, leg])
            tile = slots[0]
            for i in range(1, size):
                tile = tile + slots[i]
        return [
            jnp.broadcast_to(tile[0:vecs, d : d + 1], (vecs, lanes)) for d in range(len(dots))
        ]

    drain(field.at[0], vec_sem.at[1])
    sent = [halo_copies(0, 0)]
    for copy in sent[0]:
        copy.start()
    drain(level, level_sem.at[1])

    def look_up(m, carry):
        ids = level[m]
        energy = jnp.full(ids.shape, values[0] - mean, jnp.float32)
        for i in range(1, len(values)):
            energy = jnp.where(ids == i, values[i] - mean, energy)
        onsite[m] = energy * inv_width
        return carry

    lax.fori_loop(0, GROUP, look_up, 0)

    def arrive(copies):
        for copy in copies:
            copy.wait_recv()

    dots = [None]
    for k in range(HALF):
        arrive(sent[k])
        if k == 0:
            rule = lambda applied, here, old: applied
        else:
            rule = lambda applied, here, old: 2.0 * applied - old
        sums, copies = step(k, k + 1, k - 1 if k else None, k, rule, extra=k == 0)
        sent.append(copies)
        if k == 0:
            dots[0] = sums[2]
        dots.append(sums[0])
        dots.append(sums[1])
        if k + 1 <= RETURNED:
            give_back(k + 1)

    totals = reduce_all(dots, 0)
    nu, diag, offd, vectors = phase_one(totals, HALF, jnp.sqrt)
    arrive(sent[HALF])
    old_at, new_at = HALF + 1, HALF + 2

    def mix(coefficients, read):
        total = coefficients[0] * read(0)
        for k in range(1, len(coefficients)):
            total = total + coefficients[k] * read(k)
        return total

    which = jnp.full((1, lanes), my_vec, jnp.int32)

    def pick(value):
        row = value[0:1]
        for v in range(1, vecs):
            row = jnp.where(which == v, value[v : v + 1], row)
        return row

    old_mix = [pick(x) for x in vectors[HALF - 1][:HALF]]
    new_mix = [pick(x) for x in vectors[HALF]]
    for side in range(2):
        halo[HALF, side] = mix(new_mix, lambda k: halo[k, side])

    def restart(m, total):
        field[old_at, m] = mix(old_mix, lambda k: field[k, m])
        new = mix(new_mix, lambda k: field[k, m])
        field[new_at, m] = new
        return total + tile_sum(new * new)

    dots = [lax.fori_loop(0, GROUP, restart, jnp.zeros((8, lanes), jnp.float32))]
    gain = pick(1.0 / offd[HALF - 1])
    shift = pick(diag[HALF - 1])

    def rule(applied, here, old):
        return gain * (applied - shift * here) - old

    for k in range(HALF):
        at = HALF + k
        if k:
            arrive(sent[at])
        last = k == HALF - 1
        sums, copies = step(new_at + k, None if last else new_at + k + 1, new_at + k - 1, at, rule)
        sent.append(copies)
        dots.append(sums[0])
        if not last:
            dots.append(sums[1])

    totals = reduce_all(dots, 1)
    diag, offd = phase_two(totals, diag, offd, HALF, jnp.sqrt)
    diag = [width * a + mean for a in diag]
    offd = [width * b for b in offd]
    third, moments = chebyshev(diag, offd, nu, mean, width)

    for k in range(RETURNED):
        drain(back.at[k], back_recv.at[k])
    for v in range(vecs):
        cheb[v, 0] = mix([x[v : v + 1] for x in third], lambda k: own[v] if k == 0 else back[k - 1, v])

    for ref, items in ((diag_out, diag), (offd_out, offd), (moments_out, moments)):
        at = lax.broadcasted_iota(jnp.int32, ref.shape, 1)
        value = jnp.zeros(ref.shape, jnp.float32)
        for i, item in enumerate(items):
            value = jnp.where(at == i, item[:, : ref.shape[1]], value)
        ref[...] = value

    for copies in sent:
        for copy in copies:
            copy.wait_send()
    drain(field.at[0, pl.ds(0, GROUP - 1)], vec_sem.at[0])
    drain(level.at[pl.ds(0, GROUP - 1)], level_sem.at[0])
    for k in range(RETURNED):
        drain(field.at[k + 1, pl.ds(0, GROUP - 1), pl.ds(GHOST, rows)], back_send.at[k])
    for turn in range(2):
        drain(part.at[turn, pl.ds(0, GROUP - 1)], red_send.at[turn, 0])
        drain(part_far.at[turn, pl.ds(0, groups - 1)], red_send.at[turn, 1])


def shards(count, start_vectors, levels, energies):
    vecs, _, height, lanes = start_vectors.shape
    groups = count // GROUP
    deep = height // (GROUP // vecs) + 2 * GHOST
    f32 = jnp.float32
    vmem = pl.BlockSpec(memory_space=pltpu.VMEM)
    anywhere = pl.BlockSpec(memory_space=pl.ANY)
    dma = pltpu.SemaphoreType.DMA
    return pl.pallas_call(
        functools.partial(kernel, count),
        out_shape=(
            jax.ShapeDtypeStruct(start_vectors.shape, f32),
            jax.ShapeDtypeStruct((vecs, LANCZOS), f32),
            jax.ShapeDtypeStruct((vecs, LANCZOS - 1), f32),
            jax.ShapeDtypeStruct((vecs, 6), f32),
        ),
        in_specs=[pl.BlockSpec(memory_space=pltpu.SMEM), anywhere, anywhere],
        out_specs=(vmem,) * 4,
        scratch_shapes=[
            pltpu.VMEM((vecs, height, lanes), f32),
            pltpu.VMEM((height, lanes), jnp.int32),
            pltpu.VMEM((LANCZOS + 2, GROUP, deep, lanes), f32),
            pltpu.VMEM((LANCZOS, 2, deep, lanes), f32),
            pltpu.VMEM((GROUP, deep, lanes), f32),
            pltpu.VMEM((GROUP, deep, lanes), jnp.int32),
            pltpu.VMEM((RETURNED, vecs, height, lanes), f32),
            pltpu.VMEM((2, GROUP, 8, 128), f32),
            pltpu.VMEM((2, groups, 8, 128), f32),
            pltpu.VMEM((2, 2, 8, 128), f32),
            dma((2,)),
            dma((2,)),
            dma((2,)),
            dma((LANCZOS, 2)),
            dma((LANCZOS, 2)),
            dma((RETURNED,)),
            dma((RETURNED,)),
            dma((2, 2)),
            dma((2, 2)),
        ],
        compiler_params=pltpu.CompilerParams(
            collective_id=0, has_side_effects=True, vmem_limit_bytes=67043328
        ),
    )(energies, start_vectors, levels)


def solution(mesh):
    in_specs = (P(None, "slab", None, None), P("slab", None, None), P())
    out_specs = (P(None, "slab", None, None), P(), P(), P())
    return jax.shard_map(
        functools.partial(shards, mesh.shape["slab"]),
        mesh=mesh, in_specs=in_specs, out_specs=out_specs, check_vma=False,
    )
```

```python
import functools

import jax
import jax.numpy as jnp
from jax import lax
from jax.experimental import pallas as pl
from jax.experimental.pallas import tpu as pltpu
from jax.sharding import PartitionSpec as P

LANCZOS = 8
HALF = LANCZOS // 2
GROUP = 8
GHOST = 8
RETURNED = 3


def phase_one(dots, half, sqrt):
    norm = dots[0]
    nu = [None] * len(dots)
    nu[0] = norm / norm
    nu[1] = dots[1] / norm
    for k in range(2, len(dots)):
        nu[k] = 2.0 * dots[k] / norm - nu[k % 2]
    top = len(nu) - 1
    row, before = list(nu), None
    diag, offd = [], []
    for k in range(half):
        if k == 0:
            alpha = row[1]
        else:
            alpha = (0.5 * row[k + 1] - offd[-1] * before[k]) / row[k]
        diag.append(alpha)
        new = [None] * len(nu)
        for l in range(k + 1, top - k):
            new[l] = 0.5 * (row[l + 1] + row[l - 1]) - alpha * row[l]
            if k:
                new[l] = new[l] - offd[-1] * before[l]
        beta = sqrt(new[k + 1] / (row[k] if k == 0 else 2.0 * row[k]))
        offd.append(beta)
        inv = 1.0 / beta
        before, row = row, [None if x is None else x * inv for x in new]
    zero = nu[0] * 0.0
    scale = 1.0 / sqrt(norm)
    vectors = [[scale] + [zero] * half]
    for k in range(half):
        now = vectors[-1]
        inv = 1.0 / offd[k]
        shifted = [zero] * (half + 1)
        for l in range(k + 1):
            if l == 0:
                shifted[1] = shifted[1] + now[0]
            else:
                shifted[l + 1] = shifted[l + 1] + 0.5 * now[l]
                shifted[l - 1] = shifted[l - 1] + 0.5 * now[l]
        new = [shifted[l] - diag[k] * now[l] for l in range(half + 1)]
        if k:
            new = [x - offd[k - 1] * y for x, y in zip(new, vectors[-2])]
        vectors.append([x * inv for x in new])
    return nu, diag, offd, vectors


def phase_two(dots, diag, offd, half, sqrt):
    count = len(dots)
    gram = {}
    for k, value in enumerate(dots):
        gram[(half + k // 2, half + (k + 1) // 2)] = value
    zero = dots[0] * 0.0
    one = zero + 1.0
    for k in range(half):
        gram[(k, half)] = zero
        gram[(k, half - 1)] = one if k == half - 1 else zero
    guess_a, guess_b = diag[half - 1], offd[half - 1]
    inv = 1.0 / guess_b

    def entry(i, j):
        if (i, j) in gram:
            return gram[(i, j)]
        if j > half and i < half and (j - half) < (half - i) + 1:
            value = zero
        elif i >= half:
            value = entry(i + 1, j - 1) + entry(i - 1, j - 1) - entry(i, j - 2)
        else:
            value = (offd[i] * inv) * entry(i + 1, j - 1) - entry(i, j - 2)
            if i != half - 1:
                value = value + ((diag[i] - guess_a) * inv) * entry(i, j - 1)
            if i > 0:
                value = value + (offd[i - 1] * inv) * entry(i - 1, j - 1)
        gram[(i, j)] = value
        return value

    top = half + count - 1
    row = {l: entry(half, l) for l in range(half, top + 1)}
    before = {l: entry(half - 1, l) for l in range(half, top)}
    diag, offd = list(diag), list(offd)
    for k in range(half, 2 * half):
        if k == half:
            alpha = guess_a + guess_b * row[k + 1] / row[k]
        else:
            alpha = guess_a + (guess_b * row[k + 1] - offd[k - 1] * before[k]) / row[k]
        diag.append(alpha)
        if k == 2 * half - 1:
            break
        new = {}
        for l in range(k + 1, top - (k - half)):
            new[l] = guess_b * (row[l + 1] + row[l - 1]) + (guess_a - alpha) * row[l] - offd[k - 1] * before[l]
        beta = sqrt(new[k + 1] * guess_b / row[k])
        offd.append(beta)
        inv_b = 1.0 / beta
        before, row = row, {l: x * inv_b for l, x in new.items()}
    return diag, offd


def chebyshev(diag, offd, nu, centre, width):
    left = [None] + offd
    right = offd + [None]
    low, high = None, None
    for a, b, c in zip(diag, left, right):
        reach = b if c is None else c if b is None else b + c
        low = a - reach if low is None else jnp.minimum(low, a - reach)
        high = a + reach if high is None else jnp.maximum(high, a + reach)
    inv = 1.0 / (0.55 * (high - low))
    al = width * inv
    be = (centre - 0.5 * (high + low)) * inv
    p, q, r = 2.0 * be * be + al * al - 1.0, 4.0 * al * be, al * al
    first = [be, al]
    second = [p, q, r]
    third = [2.0 * be * p + al * q - be, 2.0 * be * q + al * (2.0 * p + r) - al, 2.0 * be * r + al * q, al * r]

    def dot(f, g):
        total = None
        for i, x in enumerate(f):
            for j, y in enumerate(g):
                term = (x * y) * (0.5 * (nu[i + j] + nu[abs(i - j)]))
                total = term if total is None else total + term
        return total

    start = [nu[0]]
    m1 = dot(start, first)
    moments = [
        m1,
        dot(start, second),
        dot(start, third),
        2.0 * dot(second, second) - 1.0,
        2.0 * dot(third, second) - m1,
        2.0 * dot(third, third) - 1.0,
    ]
    return third, moments


def kernel(
    count, energies, start, levels, cheb, diag_out, offd_out, moments_out,
    own, own_levels, field, halo, onsite, level, back, part, part_far, mine,
    load_sem, vec_sem, level_sem, halo_send, halo_recv, back_send, back_recv, red_send, red_recv,
):
    me = lax.axis_index("slab")
    member = lax.rem(me, GROUP)
    group = me // GROUP
    base = me - member
    groups = count // GROUP
    vecs, _, height, lanes = start.shape
    my_vec, block = lax.rem(member, vecs), member // vecs
    rows = height // (GROUP // vecs)
    deep = rows + 2 * GHOST
    mesh_id = pl.DeviceIdType.MESH
    ahead = lax.rem(me + GROUP, count)
    behind = lax.rem(me + count - GROUP, count)

    loads = [
        pltpu.make_async_copy(start.at[:, 0], own, load_sem.at[0]),
        pltpu.make_async_copy(levels.at[0], own_levels, load_sem.at[1]),
    ]
    for copy in loads:
        copy.start()

    def peer(i):
        return base + lax.rem(member + i, GROUP)

    def far(i):
        return lax.rem(me + i * GROUP, count)

    barrier = pltpu.get_barrier_semaphore()

    def greet(i, carry):
        pl.semaphore_signal(barrier, inc=1, device_id=(peer(i),), device_id_type=mesh_id)
        return carry

    def greet_far(i, carry):
        pl.semaphore_signal(barrier, inc=1, device_id=(far(i),), device_id_type=mesh_id)
        return carry

    lax.fori_loop(1, GROUP, greet, 0)
    lax.fori_loop(1, groups, greet_far, 0)
    pl.semaphore_wait(barrier, GROUP - 1 + groups - 1)

    def pieces(i):
        i = i // vecs
        mid = pl.multiple_of(i * rows, 8)
        top = pl.multiple_of(lax.rem(i * rows + height - GHOST, height), 8)
        low = pl.multiple_of(lax.rem(i * rows + rows, height), 8)
        return ((mid, GHOST, rows), (top, 0, GHOST), (low, GHOST + rows, GHOST))

    def vec_refs(i):
        return [
            (own.at[lax.rem(i, vecs), pl.ds(at, size)], field.at[0, member, pl.ds(to, size)])
            for at, to, size in pieces(i)
        ]

    def level_refs(i):
        return [
            (own_levels.at[pl.ds(at, size)], level.at[member, pl.ds(to, size)])
            for at, to, size in pieces(i)
        ]

    def scatter(refs, sems):
        def body(i, carry):
            to = lax.rem(member + i, GROUP)
            for src, dst in refs(to):
                pltpu.make_async_remote_copy(
                    src_ref=src, dst_ref=dst, send_sem=sems.at[0], recv_sem=sems.at[1],
                    device_id=(base + to,), device_id_type=mesh_id,
                ).start()
            return carry

        lax.fori_loop(1, GROUP, body, 0)
        for src, dst in refs(member):
            pltpu.make_async_copy(src, dst, sems.at[1]).start()

    def drain(ref, sem):
        pltpu.make_async_copy(ref, ref, sem).wait()

    loads[0].wait()
    scatter(vec_refs, vec_sem)
    loads[1].wait()
    scatter(level_refs, level_sem)

    values = [energies[i] for i in range(energies.shape[0])]
    mean = sum(values[1:], values[0]) * (1.0 / len(values))
    spread = [(x - mean) * (x - mean) for x in values]
    spread = sum(spread[1:], spread[0]) * (1.0 / len(values))
    width = 2.0 * jnp.sqrt(jnp.full((1, lanes), spread + 6.0, jnp.float32))
    inv_width = 1.0 / width

    def halo_copies(slot, at):
        part_of = pl.ds(GHOST, rows) if at == LANCZOS - 1 else pl.ds(0, deep)
        return [
            pltpu.make_async_remote_copy(
                src_ref=field.at[slot, plane, part_of], dst_ref=halo.at[at, side, part_of],
                send_sem=halo_send.at[at, side], recv_sem=halo_recv.at[at, side],
                device_id=(to,), device_id_type=mesh_id,
            )
            for plane, side, to in ((0, 1, behind), (GROUP - 1, 0, ahead))
        ]

    def give_back(k):
        def refs(i):
            return (
                field.at[k, i, pl.ds(GHOST, rows)],
                back.at[k - 1, my_vec, pl.ds(pl.multiple_of(block * rows, 8), rows)],
            )

        def body(i, carry):
            to = lax.rem(member + i, GROUP)
            src, dst = refs(to)
            pltpu.make_async_remote_copy(
                src_ref=src, dst_ref=dst, send_sem=back_send.at[k - 1], recv_sem=back_recv.at[k - 1],
                device_id=(base + to,), device_id_type=mesh_id,
            ).start()
            return carry

        lax.fori_loop(1, GROUP, body, 0)
        src, dst = refs(member)
        pltpu.make_async_copy(src, dst, back_recv.at[k - 1]).start()

    def tile_sum(x):
        x = x[GHOST : GHOST + rows]
        total = x[0:8]
        for i in range(8, rows, 8):
            total = total + x[i : i + 8]
        return total

    def step(source, target, before, at, combine, awaited, extra=False):
        nothing = jnp.zeros((8, lanes), jnp.float32)

        def local(m, here, *beside):
            near = pltpu.roll(here, 1, 0) + pltpu.roll(here, deep - 1, 0)
            near = near + pltpu.roll(here, 1, 1) + pltpu.roll(here, lanes - 1, 1)
            for plane in beside:
                near = near + field[source, plane]
            return onsite[m] * here - inv_width * near

        def finish(m, here, applied):
            new = combine(applied, here, None if before is None else field[before, m])
            if target is not None:
                field[target, m] = new
            return new

        def add(sums, here, new):
            sums = list(sums)
            sums[0] = sums[0] + tile_sum(here * new)
            sums[1] = sums[1] + tile_sum(new * new)
            if extra:
                sums[2] = sums[2] + tile_sum(here * here)
            return tuple(sums)

        def plane(m, sums):
            here = field[source, m]
            return add(sums, here, finish(m, here, local(m, here, m - 1, m + 1)))

        faces = ((0, 1), (GROUP - 1, GROUP - 2))
        parts = [local(m, field[source, m], inner) for m, inner in faces]
        for copy in awaited:
            copy.wait_recv()
        news = [
            finish(m, field[source, m], part - inv_width * halo[at, side])
            for side, ((m, inner), part) in enumerate(zip(faces, parts))
        ]
        sent = []
        if target is not None:
            sent = halo_copies(target, at + 1)
            for copy in sent:
                copy.start()
        sums = (nothing,) * 3
        for (m, inner), new in zip(faces, news):
            sums = add(sums, field[source, m], new)
        sums = lax.fori_loop(
            1,
            GROUP - 1,
            plane,
            sums,
        )
        return sums, sent

    lane = lax.broadcasted_iota(jnp.int32, (8, 128), 1)
    line = lax.broadcasted_iota(jnp.int32, (8, 128), 0)

    def reduce_all(dots, turn):
        tile = jnp.zeros((8, 128), jnp.float32)
        for d, value in enumerate(dots):
            whole = jnp.sum(jnp.sum(value, axis=0, keepdims=True), axis=1, keepdims=True)
            tile = jnp.where((lane == d) & (line == my_vec), whole, tile)
        for leg, (slots, index, size, target) in enumerate(
            ((part.at[turn], member, GROUP, peer), (part_far.at[turn], group, groups, far))
        ):
            mine[turn, leg] = tile
            slots[index] = tile

            def body(i, carry):
                pltpu.make_async_remote_copy(
                    src_ref=mine.at[turn, leg], dst_ref=slots.at[index],
                    send_sem=red_send.at[turn, leg], recv_sem=red_recv.at[turn, leg],
                    device_id=(target(i),), device_id_type=mesh_id,
                ).start()
                return carry

            lax.fori_loop(1, size, body, 0)
            drain(slots.at[pl.ds(0, size - 1)], red_recv.at[turn, leg])
            tile = slots[0]
            for i in range(1, size):
                tile = tile + slots[i]
        return [
            jnp.broadcast_to(tile[0:vecs, d : d + 1], (vecs, lanes)) for d in range(len(dots))
        ]

    drain(field.at[0], vec_sem.at[1])
    sent = [halo_copies(0, 0)]
    for copy in sent[0]:
        copy.start()
    drain(level, level_sem.at[1])

    def look_up(m, carry):
        ids = level[m]
        energy = jnp.full(ids.shape, values[0] - mean, jnp.float32)
        for i in range(1, len(values)):
            energy = jnp.where(ids == i, values[i] - mean, energy)
        onsite[m] = energy * inv_width
        return carry

    lax.fori_loop(0, GROUP, look_up, 0)

    def arrive(copies):
        for copy in copies:
            copy.wait_recv()

    dots = [None]
    for k in range(HALF):
        if k == 0:
            rule = lambda applied, here, old: applied
        else:
            rule = lambda applied, here, old: 2.0 * applied - old
        sums, copies = step(k, k + 1, k - 1 if k else None, k, rule, sent[k], extra=k == 0)
        sent.append(copies)
        if k == 0:
            dots[0] = sums[2]
        dots.append(sums[0])
        dots.append(sums[1])
        if k + 1 <= RETURNED:
            give_back(k + 1)

    totals = reduce_all(dots, 0)
    nu, diag, offd, vectors = phase_one(totals, HALF, jnp.sqrt)
    arrive(sent[HALF])
    old_at, new_at = HALF + 1, HALF + 2

    def mix(coefficients, read):
        total = coefficients[0] * read(0)
        for k in range(1, len(coefficients)):
            total = total + coefficients[k] * read(k)
        return total

    which = jnp.full((1, lanes), my_vec, jnp.int32)

    def pick(value):
        row = value[0:1]
        for v in range(1, vecs):
            row = jnp.where(which == v, value[v : v + 1], row)
        return row

    old_mix = [pick(x) for x in vectors[HALF - 1][:HALF]]
    new_mix = [pick(x) for x in vectors[HALF]]
    for side in range(2):
        halo[HALF, side] = mix(new_mix, lambda k: halo[k, side])

    def restart(m, total):
        field[old_at, m] = mix(old_mix, lambda k: field[k, m])
        new = mix(new_mix, lambda k: field[k, m])
        field[new_at, m] = new
        return total + tile_sum(new * new)

    dots = [lax.fori_loop(0, GROUP, restart, jnp.zeros((8, lanes), jnp.float32))]
    gain = pick(1.0 / offd[HALF - 1])
    shift = pick(diag[HALF - 1])

    def rule(applied, here, old):
        return gain * (applied - shift * here) - old

    for k in range(HALF):
        at = HALF + k
        last = k == HALF - 1
        sums, copies = step(new_at + k, None if last else new_at + k + 1, new_at + k - 1, at, rule, sent[at] if k else [])
        sent.append(copies)
        dots.append(sums[0])
        if not last:
            dots.append(sums[1])

    totals = reduce_all(dots, 1)
    diag, offd = phase_two(totals, diag, offd, HALF, jnp.sqrt)
    diag = [width * a + mean for a in diag]
    offd = [width * b for b in offd]
    third, moments = chebyshev(diag, offd, nu, mean, width)

    for k in range(RETURNED):
        drain(back.at[k], back_recv.at[k])
    for v in range(vecs):
        cheb[v, 0] = mix([x[v : v + 1] for x in third], lambda k: own[v] if k == 0 else back[k - 1, v])

    for ref, items in ((diag_out, diag), (offd_out, offd), (moments_out, moments)):
        at = lax.broadcasted_iota(jnp.int32, ref.shape, 1)
        value = jnp.zeros(ref.shape, jnp.float32)
        for i, item in enumerate(items):
            value = jnp.where(at == i, item[:, : ref.shape[1]], value)
        ref[...] = value

    for copies in sent:
        for copy in copies:
            copy.wait_send()
    drain(field.at[0, pl.ds(0, GROUP - 1)], vec_sem.at[0])
    drain(level.at[pl.ds(0, GROUP - 1)], level_sem.at[0])
    for k in range(RETURNED):
        drain(field.at[k + 1, pl.ds(0, GROUP - 1), pl.ds(GHOST, rows)], back_send.at[k])
    for turn in range(2):
        drain(part.at[turn, pl.ds(0, GROUP - 1)], red_send.at[turn, 0])
        drain(part_far.at[turn, pl.ds(0, groups - 1)], red_send.at[turn, 1])


def shards(count, start_vectors, levels, energies):
    vecs, _, height, lanes = start_vectors.shape
    groups = count // GROUP
    deep = height // (GROUP // vecs) + 2 * GHOST
    f32 = jnp.float32
    vmem = pl.BlockSpec(memory_space=pltpu.VMEM)
    anywhere = pl.BlockSpec(memory_space=pl.ANY)
    dma = pltpu.SemaphoreType.DMA
    return pl.pallas_call(
        functools.partial(kernel, count),
        out_shape=(
            jax.ShapeDtypeStruct(start_vectors.shape, f32),
            jax.ShapeDtypeStruct((vecs, LANCZOS), f32),
            jax.ShapeDtypeStruct((vecs, LANCZOS - 1), f32),
            jax.ShapeDtypeStruct((vecs, 6), f32),
        ),
        in_specs=[pl.BlockSpec(memory_space=pltpu.SMEM), anywhere, anywhere],
        out_specs=(vmem,) * 4,
        scratch_shapes=[
            pltpu.VMEM((vecs, height, lanes), f32),
            pltpu.VMEM((height, lanes), jnp.int32),
            pltpu.VMEM((LANCZOS + 2, GROUP, deep, lanes), f32),
            pltpu.VMEM((LANCZOS, 2, deep, lanes), f32),
            pltpu.VMEM((GROUP, deep, lanes), f32),
            pltpu.VMEM((GROUP, deep, lanes), jnp.int32),
            pltpu.VMEM((RETURNED, vecs, height, lanes), f32),
            pltpu.VMEM((2, GROUP, 8, 128), f32),
            pltpu.VMEM((2, groups, 8, 128), f32),
            pltpu.VMEM((2, 2, 8, 128), f32),
            dma((2,)),
            dma((2,)),
            dma((2,)),
            dma((LANCZOS, 2)),
            dma((LANCZOS, 2)),
            dma((RETURNED,)),
            dma((RETURNED,)),
            dma((2, 2)),
            dma((2, 2)),
        ],
        compiler_params=pltpu.CompilerParams(
            collective_id=0, has_side_effects=True, vmem_limit_bytes=67043328
        ),
    )(energies, start_vectors, levels)


def solution(mesh):
    in_specs = (P(None, "slab", None, None), P("slab", None, None), P())
    out_specs = (P(None, "slab", None, None), P(), P(), P())
    return jax.shard_map(
        functools.partial(shards, mesh.shape["slab"]),
        mesh=mesh, in_specs=in_specs, out_specs=out_specs, check_vma=False,
    )
```

```python
import functools

import jax
import jax.numpy as jnp
from jax import lax
from jax.experimental import pallas as pl
from jax.experimental.pallas import tpu as pltpu
from jax.sharding import PartitionSpec as P

LANCZOS = 8
HALF = LANCZOS // 2
GROUP = 8
GHOST = 8
RETURNED = 3


def phase_one(dots, half, sqrt):
    norm = dots[0]
    nu = [None] * len(dots)
    nu[0] = norm / norm
    nu[1] = dots[1] / norm
    for k in range(2, len(dots)):
        nu[k] = 2.0 * dots[k] / norm - nu[k % 2]
    top = len(nu) - 1
    row, before = list(nu), None
    diag, offd = [], []
    for k in range(half):
        if k == 0:
            alpha = row[1]
        else:
            alpha = (0.5 * row[k + 1] - offd[-1] * before[k]) / row[k]
        diag.append(alpha)
        new = [None] * len(nu)
        for l in range(k + 1, top - k):
            new[l] = 0.5 * (row[l + 1] + row[l - 1]) - alpha * row[l]
            if k:
                new[l] = new[l] - offd[-1] * before[l]
        beta = sqrt(new[k + 1] / (row[k] if k == 0 else 2.0 * row[k]))
        offd.append(beta)
        inv = 1.0 / beta
        before, row = row, [None if x is None else x * inv for x in new]
    zero = nu[0] * 0.0
    scale = 1.0 / sqrt(norm)
    vectors = [[scale] + [zero] * half]
    for k in range(half):
        now = vectors[-1]
        inv = 1.0 / offd[k]
        shifted = [zero] * (half + 1)
        for l in range(k + 1):
            if l == 0:
                shifted[1] = shifted[1] + now[0]
            else:
                shifted[l + 1] = shifted[l + 1] + 0.5 * now[l]
                shifted[l - 1] = shifted[l - 1] + 0.5 * now[l]
        new = [shifted[l] - diag[k] * now[l] for l in range(half + 1)]
        if k:
            new = [x - offd[k - 1] * y for x, y in zip(new, vectors[-2])]
        vectors.append([x * inv for x in new])
    return nu, diag, offd, vectors


def phase_two(dots, diag, offd, half, sqrt):
    count = len(dots)
    gram = {}
    for k, value in enumerate(dots):
        gram[(half + k // 2, half + (k + 1) // 2)] = value
    zero = dots[0] * 0.0
    one = zero + 1.0
    for k in range(half):
        gram[(k, half)] = zero
        gram[(k, half - 1)] = one if k == half - 1 else zero
    guess_a, guess_b = diag[half - 1], offd[half - 1]
    inv = 1.0 / guess_b

    def entry(i, j):
        if (i, j) in gram:
            return gram[(i, j)]
        if j > half and i < half and (j - half) < (half - i) + 1:
            value = zero
        elif i >= half:
            value = entry(i + 1, j - 1) + entry(i - 1, j - 1) - entry(i, j - 2)
        else:
            value = (offd[i] * inv) * entry(i + 1, j - 1) - entry(i, j - 2)
            if i != half - 1:
                value = value + ((diag[i] - guess_a) * inv) * entry(i, j - 1)
            if i > 0:
                value = value + (offd[i - 1] * inv) * entry(i - 1, j - 1)
        gram[(i, j)] = value
        return value

    top = half + count - 1
    row = {l: entry(half, l) for l in range(half, top + 1)}
    before = {l: entry(half - 1, l) for l in range(half, top)}
    diag, offd = list(diag), list(offd)
    for k in range(half, 2 * half):
        if k == half:
            alpha = guess_a + guess_b * row[k + 1] / row[k]
        else:
            alpha = guess_a + (guess_b * row[k + 1] - offd[k - 1] * before[k]) / row[k]
        diag.append(alpha)
        if k == 2 * half - 1:
            break
        new = {}
        for l in range(k + 1, top - (k - half)):
            new[l] = guess_b * (row[l + 1] + row[l - 1]) + (guess_a - alpha) * row[l] - offd[k - 1] * before[l]
        beta = sqrt(new[k + 1] * guess_b / row[k])
        offd.append(beta)
        inv_b = 1.0 / beta
        before, row = row, {l: x * inv_b for l, x in new.items()}
    return diag, offd


def chebyshev(diag, offd, nu, centre, width):
    left = [None] + offd
    right = offd + [None]
    low, high = None, None
    for a, b, c in zip(diag, left, right):
        reach = b if c is None else c if b is None else b + c
        low = a - reach if low is None else jnp.minimum(low, a - reach)
        high = a + reach if high is None else jnp.maximum(high, a + reach)
    inv = 1.0 / (0.55 * (high - low))
    al = width * inv
    be = (centre - 0.5 * (high + low)) * inv
    p, q, r = 2.0 * be * be + al * al - 1.0, 4.0 * al * be, al * al
    first = [be, al]
    second = [p, q, r]
    third = [2.0 * be * p + al * q - be, 2.0 * be * q + al * (2.0 * p + r) - al, 2.0 * be * r + al * q, al * r]

    def dot(f, g):
        total = None
        for i, x in enumerate(f):
            for j, y in enumerate(g):
                term = (x * y) * (0.5 * (nu[i + j] + nu[abs(i - j)]))
                total = term if total is None else total + term
        return total

    start = [nu[0]]
    m1 = dot(start, first)
    moments = [
        m1,
        dot(start, second),
        dot(start, third),
        2.0 * dot(second, second) - 1.0,
        2.0 * dot(third, second) - m1,
        2.0 * dot(third, third) - 1.0,
    ]
    return third, moments


def kernel(
    count, energies, start, levels, cheb, diag_out, offd_out, moments_out,
    own, own_levels, field, halo, onsite, level, back, part, part_far, mine,
    load_sem, vec_sem, level_sem, halo_send, halo_recv, back_send, back_recv, red_send, red_recv,
):
    me = lax.axis_index("slab")
    member = lax.rem(me, GROUP)
    group = me // GROUP
    base = me - member
    groups = count // GROUP
    vecs, _, height, lanes = start.shape
    my_vec, block = lax.rem(member, vecs), member // vecs
    rows = height // (GROUP // vecs)
    deep = rows + 2 * GHOST
    mesh_id = pl.DeviceIdType.MESH
    ahead = lax.rem(me + GROUP, count)
    behind = lax.rem(me + count - GROUP, count)

    loads = [
        pltpu.make_async_copy(start.at[:, 0], own, load_sem.at[0]),
        pltpu.make_async_copy(levels.at[0], own_levels, load_sem.at[1]),
    ]
    for copy in loads:
        copy.start()

    def peer(i):
        return base + lax.rem(member + i, GROUP)

    def far(i):
        return lax.rem(me + i * GROUP, count)

    barrier = pltpu.get_barrier_semaphore()

    def greet(i, carry):
        pl.semaphore_signal(barrier, inc=1, device_id=(peer(i),), device_id_type=mesh_id)
        return carry

    def greet_far(i, carry):
        pl.semaphore_signal(barrier, inc=1, device_id=(far(i),), device_id_type=mesh_id)
        return carry

    lax.fori_loop(1, GROUP, greet, 0)
    lax.fori_loop(1, groups, greet_far, 0)
    pl.semaphore_wait(barrier, GROUP - 1 + groups - 1)

    def pieces(i):
        i = i // vecs
        mid = pl.multiple_of(i * rows, 8)
        top = pl.multiple_of(lax.rem(i * rows + height - GHOST, height), 8)
        low = pl.multiple_of(lax.rem(i * rows + rows, height), 8)
        return ((mid, GHOST, rows), (top, 0, GHOST), (low, GHOST + rows, GHOST))

    def vec_refs(i):
        return [
            (own.at[lax.rem(i, vecs), pl.ds(at, size)], field.at[0, member, pl.ds(to, size)])
            for at, to, size in pieces(i)
        ]

    def level_refs(i):
        return [
            (own_levels.at[pl.ds(at, size)], level.at[member, pl.ds(to, size)])
            for at, to, size in pieces(i)
        ]

    def scatter(refs, sems):
        def body(i, carry):
            to = lax.rem(member + i, GROUP)
            for src, dst in refs(to):
                pltpu.make_async_remote_copy(
                    src_ref=src, dst_ref=dst, send_sem=sems.at[0], recv_sem=sems.at[1],
                    device_id=(base + to,), device_id_type=mesh_id,
                ).start()
            return carry

        lax.fori_loop(1, GROUP, body, 0)
        for src, dst in refs(member):
            pltpu.make_async_copy(src, dst, sems.at[1]).start()

    def drain(ref, sem):
        pltpu.make_async_copy(ref, ref, sem).wait()

    loads[0].wait()
    scatter(vec_refs, vec_sem)
    loads[1].wait()
    scatter(level_refs, level_sem)

    values = [energies[i] for i in range(energies.shape[0])]
    mean = sum(values[1:], values[0]) * (1.0 / len(values))
    spread = [(x - mean) * (x - mean) for x in values]
    spread = sum(spread[1:], spread[0]) * (1.0 / len(values))
    width = 2.0 * jnp.sqrt(jnp.full((1, lanes), spread + 6.0, jnp.float32))
    inv_width = 1.0 / width

    def halo_copies(slot, at):
        part_of = pl.ds(GHOST, rows) if at == LANCZOS - 1 else pl.ds(0, deep)
        return [
            pltpu.make_async_remote_copy(
                src_ref=field.at[slot, plane, part_of], dst_ref=halo.at[at, side, part_of],
                send_sem=halo_send.at[at, side], recv_sem=halo_recv.at[at, side],
                device_id=(to,), device_id_type=mesh_id,
            )
            for plane, side, to in ((0, 1, behind), (GROUP - 1, 0, ahead))
        ]

    def give_back(k):
        def refs(i):
            return (
                field.at[k, i, pl.ds(GHOST, rows)],
                back.at[k - 1, my_vec, pl.ds(pl.multiple_of(block * rows, 8), rows)],
            )

        def body(i, carry):
            to = lax.rem(member + i, GROUP)
            src, dst = refs(to)
            pltpu.make_async_remote_copy(
                src_ref=src, dst_ref=dst, send_sem=back_send.at[k - 1], recv_sem=back_recv.at[k - 1],
                device_id=(base + to,), device_id_type=mesh_id,
            ).start()
            return carry

        lax.fori_loop(1, GROUP, body, 0)
        src, dst = refs(member)
        pltpu.make_async_copy(src, dst, back_recv.at[k - 1]).start()

    def tile_sum(x):
        x = x[GHOST : GHOST + rows]
        total = x[0:8]
        for i in range(8, rows, 8):
            total = total + x[i : i + 8]
        return total

    def step(source, target, before, at, combine, awaited, extra=False):
        nothing = jnp.zeros((8, lanes), jnp.float32)

        def local(m, here, *beside):
            near = pltpu.roll(here, 1, 0) + pltpu.roll(here, deep - 1, 0)
            near = near + pltpu.roll(here, 1, 1) + pltpu.roll(here, lanes - 1, 1)
            for plane in beside:
                near = near + field[source, plane]
            return onsite[m] * here - inv_width * near

        def finish(m, here, applied):
            new = combine(applied, here, None if before is None else field[before, m])
            if target is not None:
                field[target, m] = new
            return new

        def add(sums, here, new):
            sums = list(sums)
            sums[0] = sums[0] + tile_sum(here * new)
            sums[1] = sums[1] + tile_sum(new * new)
            if extra:
                sums[2] = sums[2] + tile_sum(here * here)
            return tuple(sums)

        def plane(m, sums):
            here = field[source, m]
            return add(sums, here, finish(m, here, local(m, here, m - 1, m + 1)))

        faces = ((0, 1), (GROUP - 1, GROUP - 2))
        parts = [local(m, field[source, m], inner) for m, inner in faces]
        for copy in awaited:
            copy.wait_recv()
        news = [
            finish(m, field[source, m], part - inv_width * halo[at, side])
            for side, ((m, inner), part) in enumerate(zip(faces, parts))
        ]
        sent = []
        if target is not None:
            sent = halo_copies(target, at + 1)
            for copy in sent:
                copy.start()
        sums = (nothing,) * 3
        for (m, inner), new in zip(faces, news):
            sums = add(sums, field[source, m], new)
        sums = lax.fori_loop(
            1,
            GROUP - 1,
            plane,
            sums,
            unroll=3,
        )
        return sums, sent

    lane = lax.broadcasted_iota(jnp.int32, (8, 128), 1)
    line = lax.broadcasted_iota(jnp.int32, (8, 128), 0)

    def reduce_all(dots, turn):
        tile = jnp.zeros((8, 128), jnp.float32)
        for d, value in enumerate(dots):
            whole = jnp.sum(jnp.sum(value, axis=0, keepdims=True), axis=1, keepdims=True)
            tile = jnp.where((lane == d) & (line == my_vec), whole, tile)
        for leg, (slots, index, size, target) in enumerate(
            ((part.at[turn], member, GROUP, peer), (part_far.at[turn], group, groups, far))
        ):
            mine[turn, leg] = tile
            slots[index] = tile

            def body(i, carry):
                pltpu.make_async_remote_copy(
                    src_ref=mine.at[turn, leg], dst_ref=slots.at[index],
                    send_sem=red_send.at[turn, leg], recv_sem=red_recv.at[turn, leg],
                    device_id=(target(i),), device_id_type=mesh_id,
                ).start()
                return carry

            lax.fori_loop(1, size, body, 0)
            drain(slots.at[pl.ds(0, size - 1)], red_recv.at[turn, leg])
            tile = slots[0]
            for i in range(1, size):
                tile = tile + slots[i]
        return [
            jnp.broadcast_to(tile[0:vecs, d : d + 1], (vecs, lanes)) for d in range(len(dots))
        ]

    drain(field.at[0], vec_sem.at[1])
    sent = [halo_copies(0, 0)]
    for copy in sent[0]:
        copy.start()
    drain(level, level_sem.at[1])

    def look_up(m, carry):
        ids = level[m]
        energy = jnp.full(ids.shape, values[0] - mean, jnp.float32)
        for i in range(1, len(values)):
            energy = jnp.where(ids == i, values[i] - mean, energy)
        onsite[m] = energy * inv_width
        return carry

    lax.fori_loop(0, GROUP, look_up, 0)

    def arrive(copies):
        for copy in copies:
            copy.wait_recv()

    dots = [None]
    for k in range(HALF):
        if k == 0:
            rule = lambda applied, here, old: applied
        else:
            rule = lambda applied, here, old: 2.0 * applied - old
        sums, copies = step(k, k + 1, k - 1 if k else None, k, rule, sent[k], extra=k == 0)
        sent.append(copies)
        if k == 0:
            dots[0] = sums[2]
        dots.append(sums[0])
        dots.append(sums[1])
        if k + 1 <= RETURNED:
            give_back(k + 1)

    totals = reduce_all(dots, 0)
    nu, diag, offd, vectors = phase_one(totals, HALF, jnp.sqrt)
    arrive(sent[HALF])
    old_at, new_at = HALF + 1, HALF + 2

    def mix(coefficients, read):
        total = coefficients[0] * read(0)
        for k in range(1, len(coefficients)):
            total = total + coefficients[k] * read(k)
        return total

    which = jnp.full((1, lanes), my_vec, jnp.int32)

    def pick(value):
        row = value[0:1]
        for v in range(1, vecs):
            row = jnp.where(which == v, value[v : v + 1], row)
        return row

    old_mix = [pick(x) for x in vectors[HALF - 1][:HALF]]
    new_mix = [pick(x) for x in vectors[HALF]]
    for side in range(2):
        halo[HALF, side] = mix(new_mix, lambda k: halo[k, side])

    def restart(m, total):
        field[old_at, m] = mix(old_mix, lambda k: field[k, m])
        new = mix(new_mix, lambda k: field[k, m])
        field[new_at, m] = new
        return total + tile_sum(new * new)

    dots = [
        lax.fori_loop(0, GROUP, restart, jnp.zeros((8, lanes), jnp.float32), unroll=2)
    ]
    gain = pick(1.0 / offd[HALF - 1])
    shift = pick(diag[HALF - 1])

    def rule(applied, here, old):
        return gain * (applied - shift * here) - old

    for k in range(HALF):
        at = HALF + k
        last = k == HALF - 1
        sums, copies = step(new_at + k, None if last else new_at + k + 1, new_at + k - 1, at, rule, sent[at] if k else [])
        sent.append(copies)
        dots.append(sums[0])
        if not last:
            dots.append(sums[1])

    totals = reduce_all(dots, 1)
    diag, offd = phase_two(totals, diag, offd, HALF, jnp.sqrt)
    diag = [width * a + mean for a in diag]
    offd = [width * b for b in offd]
    third, moments = chebyshev(diag, offd, nu, mean, width)

    for k in range(RETURNED):
        drain(back.at[k], back_recv.at[k])
    for v in range(vecs):
        cheb[v, 0] = mix([x[v : v + 1] for x in third], lambda k: own[v] if k == 0 else back[k - 1, v])

    for ref, items in ((diag_out, diag), (offd_out, offd), (moments_out, moments)):
        at = lax.broadcasted_iota(jnp.int32, ref.shape, 1)
        value = jnp.zeros(ref.shape, jnp.float32)
        for i, item in enumerate(items):
            value = jnp.where(at == i, item[:, : ref.shape[1]], value)
        ref[...] = value

    for copies in sent:
        for copy in copies:
            copy.wait_send()
    drain(field.at[0, pl.ds(0, GROUP - 1)], vec_sem.at[0])
    drain(level.at[pl.ds(0, GROUP - 1)], level_sem.at[0])
    for k in range(RETURNED):
        drain(field.at[k + 1, pl.ds(0, GROUP - 1), pl.ds(GHOST, rows)], back_send.at[k])
    for turn in range(2):
        drain(part.at[turn, pl.ds(0, GROUP - 1)], red_send.at[turn, 0])
        drain(part_far.at[turn, pl.ds(0, groups - 1)], red_send.at[turn, 1])


def shards(count, start_vectors, levels, energies):
    vecs, _, height, lanes = start_vectors.shape
    groups = count // GROUP
    deep = height // (GROUP // vecs) + 2 * GHOST
    f32 = jnp.float32
    vmem = pl.BlockSpec(memory_space=pltpu.VMEM)
    anywhere = pl.BlockSpec(memory_space=pl.ANY)
    dma = pltpu.SemaphoreType.DMA
    return pl.pallas_call(
        functools.partial(kernel, count),
        out_shape=(
            jax.ShapeDtypeStruct(start_vectors.shape, f32),
            jax.ShapeDtypeStruct((vecs, LANCZOS), f32),
            jax.ShapeDtypeStruct((vecs, LANCZOS - 1), f32),
            jax.ShapeDtypeStruct((vecs, 6), f32),
        ),
        in_specs=[pl.BlockSpec(memory_space=pltpu.SMEM), anywhere, anywhere],
        out_specs=(vmem,) * 4,
        scratch_shapes=[
            pltpu.VMEM((vecs, height, lanes), f32),
            pltpu.VMEM((height, lanes), jnp.int32),
            pltpu.VMEM((LANCZOS + 2, GROUP, deep, lanes), f32),
            pltpu.VMEM((LANCZOS, 2, deep, lanes), f32),
            pltpu.VMEM((GROUP, deep, lanes), f32),
            pltpu.VMEM((GROUP, deep, lanes), jnp.int32),
            pltpu.VMEM((RETURNED, vecs, height, lanes), f32),
            pltpu.VMEM((2, GROUP, 8, 128), f32),
            pltpu.VMEM((2, groups, 8, 128), f32),
            pltpu.VMEM((2, 2, 8, 128), f32),
            dma((2,)),
            dma((2,)),
            dma((2,)),
            dma((LANCZOS, 2)),
            dma((LANCZOS, 2)),
            dma((RETURNED,)),
            dma((RETURNED,)),
            dma((2, 2)),
            dma((2, 2)),
        ],
        compiler_params=pltpu.CompilerParams(
            collective_id=0, has_side_effects=True, vmem_limit_bytes=67043328
        ),
    )(energies, start_vectors, levels)


def solution(mesh):
    in_specs = (P(None, "slab", None, None), P("slab", None, None), P())
    out_specs = (P(None, "slab", None, None), P(), P(), P())
    return jax.shard_map(
        functools.partial(shards, mesh.shape["slab"]),
        mesh=mesh, in_specs=in_specs, out_specs=out_specs, check_vma=False,
    )
```
